16 devices in a mesh: rep: 4 (over y, z, core), dp: 4 (over x).
Axes of the slice: x: 4, y: 2, z: 1, core: 2. Of those that a mesh axis runs over, the one named last changes fastest.
The devices are a block of a 4x4x8 slice.
Arguments:
- x: bfloat16 [16, 4096, 1024], P(('rep', 'dp')), parts along dimension 0
- dy: bfloat16 [16, 4096, 1024], P(('rep', 'dp')), parts along dimension 0
- w_gate: bfloat16 [2, 1024, 4096], P(None, 'dp')
- w_up: bfloat16 [2, 1024, 4096], P(None, 'dp')
- w_down: bfloat16 [2, 4096, 1024], P(None, 'dp')
- m_w_gate: float32 [2, 1024, 4096], P(None, 'dp')
- m_w_up: float32 [2, 1024, 4096], P(None, 'dp')
- m_w_down: float32 [2, 4096, 1024], P(None, 'dp')
- v_w_gate: float32 [2, 1024, 4096], P(None, 'dp')
- v_w_up: float32 [2, 1024, 4096], P(None, 'dp')
- v_w_down: float32 [2, 4096, 1024], P(None, 'dp')
Outputs:
- output 1: bfloat16 [8, 1024, 4096], P('rep', 'dp'), parts along dimension 0
- output 2: bfloat16 [8, 1024, 4096], P('rep', 'dp'), parts along dimension 0
- output 3: bfloat16 [8, 4096, 1024], P('rep', 'dp'), parts along dimension 0
- output 4: float32 [8, 1024, 4096], P('rep', 'dp'), parts along dimension 0
- output 5: float32 [8, 1024, 4096], P('rep', 'dp'), parts along dimension 0
- output 6: float32 [8, 4096, 1024], P('rep', 'dp'), parts along dimension 0
- output 7: float32 [8, 1024, 4096], P('rep', 'dp'), parts along dimension 0
- output 8: float32 [8, 1024, 4096], P('rep', 'dp'), parts along dimension 0
- output 9: float32 [8, 4096, 1024], P('rep', 'dp'), parts along dimension 0
There are 4 independent parts. The reference program is written for one: setup_inputs(seed, part) draws one part's arguments, and reference() takes and returns one part's arrays. A program takes and returns all parts, laid end to end along the dimension named above; an argument that names none is the same for every part.
All inputs are finite; a program needn't handle non-finite values.
Results may differ from the reference program's by a relative error of at most 0.0242.
Values are sent between devices in bfloat16 or wider.
A program may use at most 768 MiB of HBM per device.

```python
import jax
import jax.numpy as jnp
from jax import lax

SEQUENCES = 4
TOKENS = 4096
D = 1024
FF = 4096
LAYERS = 2
NAMES = ("w_gate", "w_up", "w_down")
SHAPES = {"w_gate": (LAYERS, D, FF), "w_up": (LAYERS, D, FF), "w_down": (LAYERS, FF, D)}


def bump(key, n, height):
    away = (jnp.arange(n, dtype=jnp.int32) - jax.random.randint(key, (), 0, n, jnp.int32)) % n
    return jnp.where(away < n // 8, height, 1.0)


def together(key, own, strength):
    shared = jax.random.normal(key, own.shape[1:], jnp.float32)
    return (own + strength * shared) * lax.rsqrt(1 + strength * strength)


def setup_inputs(seed: int = 0, part: int = 0) -> dict:
    kx, kdy, ka, kb, kz, kf, kh, kl, *keys = jax.random.split(jax.random.key(seed), 8 + 3 * len(NAMES))
    kx, kdy, ka, kb = (jax.random.fold_in(k, part) for k in (kx, kdy, ka, kb))
    kw, km, kv = (keys[i::3] for i in range(3))
    shape = (SEQUENCES, TOKENS, D)
    much_x, much_dy = jax.random.uniform(kz, (2,), jnp.float32, 0.0, 1.0)
    loud = 2.0 ** jax.random.uniform(jax.random.fold_in(kz, 1), (), jnp.float32, -1.0, 2.0)
    layers = 2.0 ** jax.random.uniform(kl, (LAYERS, 1, 1), jnp.float32, -1.0, 1.0)
    x = together(ka, jax.random.normal(kx, shape, jnp.float32), much_x) * bump(kf, D, 4.0)
    dy = together(kb, jax.random.normal(kdy, shape, jnp.float32), much_dy)
    drawn = {"x": x.astype(jnp.bfloat16), "dy": (loud * dy * (SEQUENCES * TOKENS) ** -0.5).astype(jnp.bfloat16)}
    for key, name in zip(kw, NAMES, strict=True):
        w = jax.random.normal(key, SHAPES[name], jnp.float32) * SHAPES[name][1] ** -0.5
        drawn[name] = (w * {"w_gate": 1.0, "w_up": bump(kh, FF, 4.0), "w_down": layers}[name]).astype(jnp.bfloat16)
    for key, name in zip(km, NAMES, strict=True):
        drawn[f"m_{name}"] = 0.1 * jax.random.normal(key, SHAPES[name], jnp.float32)
    for key, name in zip(kv, NAMES, strict=True):
        drawn[f"v_{name}"] = jax.random.uniform(key, SHAPES[name], jnp.float32, 0.005, 0.015)
    return drawn


def matmul(a, w):
    return jnp.dot(a, w, preferred_element_type=jnp.float32).astype(jnp.bfloat16)


def normed(h):
    wide = h.astype(jnp.float32)
    scale = lax.rsqrt(jnp.mean(wide**2, -1, keepdims=True) + 1e-6)
    return (wide * scale).astype(jnp.bfloat16)


def layer(h, w):
    a = normed(h)
    gate = jnp.dot(a, w["w_gate"], preferred_element_type=jnp.float32)
    up = jnp.dot(a, w["w_up"], preferred_element_type=jnp.float32)
    return h + matmul((jax.nn.silu(gate) * up).astype(jnp.bfloat16), w["w_down"])


def adamw(w, m, v, g):
    m = 0.9 * m + 0.1 * g
    v = 0.95 * v + 0.05 * g * g
    step = m * lax.rsqrt(v + 1e-8) + 0.1 * w
    return (w - 0.02 * step).astype(jnp.bfloat16), m, v


def stack(weights, h):
    return lax.scan(lambda h, w: (layer(h, w), None), h, weights)[0]


def reference(x, dy, w_gate, w_up, w_down, m_w_gate, m_w_up, m_w_down, v_w_gate, v_w_up, v_w_down):
    weights = dict(zip(NAMES, (w_gate, w_up, w_down), strict=True))

    def take(so_far, sequence):
        h, by_y = sequence
        _, back = jax.vjp(lambda w: stack(w, h), weights)
        return jax.tree.map(lambda total, term: total + term.astype(jnp.float32), so_far, back(by_y)[0]), None

    none_yet = {name: jnp.zeros(w.shape, jnp.float32) for name, w in weights.items()}
    by_weights, _ = lax.scan(take, none_yet, (x, dy))
    gradients = [by_weights[name].astype(jnp.bfloat16).astype(jnp.float32) for name in NAMES]
    new = [
        adamw(w.astype(jnp.float32), m, v, g)
        for w, m, v, g in zip((w_gate, w_up, w_down), (m_w_gate, m_w_up, m_w_down), (v_w_gate, v_w_up, v_w_down), gradients, strict=True)
    ]
    return tuple(one[which] for which in range(3) for one in new)
```

```python
import functools

import jax
import jax.numpy as jnp
from jax import lax
from jax.experimental import pallas as pl
from jax.experimental.pallas import tpu as pltpu
from jax.sharding import PartitionSpec as P

F32, BF16 = jnp.float32, jnp.bfloat16
VMEM_LIMIT = 61 * 2**20
CHUNKS = 4
LAST_RANGES = ((0, 1), (1, 2), (2, 3), (3, 4))


def dot(a, b, over_a, over_b):
    return lax.dot_general(a, b, (((over_a,), (over_b,)), ((), ())), preferred_element_type=F32)


def rounded(a):
    return a.astype(BF16).astype(F32)


def norm_scale(wide):
    return lax.rsqrt(jnp.mean(wide * wide, -1, keepdims=True) + 1e-6)


def riding(kernel, ins, outs, gather, steps, when):
    def whole(*refs):
        refs = list(refs)
        take = lambda n: [refs.pop(0) for _ in range(n)]
        mine, sources, results, gathered = take(ins), take(3), take(outs), take(gather.count)
        sems = [refs.pop(), refs.pop()]
        gather.bind(sources, gathered, sems[::-1])
        index = 0
        for axis in range(len(steps)):
            index = index * steps[axis] + pl.program_id(axis)
        total = 1
        for n in steps:
            total *= n
        pl.when(index == 0)(gather.begin)
        if when[0] < total:
            pl.when(index == when[0])(gather.pass_on)
        if when[1] < total:
            pl.when(index == when[1])(gather.pass_far)
        kernel(*mine, *results, *refs)

        @pl.when(index == total - 1)
        def _():
            if when[0] >= total:
                gather.pass_on()
            if when[1] >= total:
                gather.pass_far()
            gather.end()

    return whole


def call(kernel, grid, in_specs, out_specs, out_shape, flops, moved, scratch=(), aliases=None, name=None, gather=None, when=None, ident=None, sources=None):
    params = dict(vmem_limit_bytes=VMEM_LIMIT)
    in_specs, out_specs, out_shape, scratch = list(in_specs), out_specs, out_shape, list(scratch)
    if gather is not None:
        kernel = riding(kernel, len(in_specs), len(out_specs), gather, grid, when)
        in_specs = in_specs + [ANY] * 3
        out_specs = list(out_specs) + [ANY] * gather.count
        out_shape = list(out_shape) + gather.out_shape(sources[0].shape[1], sources[2].shape[2])
        scratch = scratch + gather.scratch()
        params.update(collective_id=ident, has_side_effects=True)
    run = pl.pallas_call(
        kernel,
        grid=grid,
        in_specs=in_specs,
        out_specs=out_specs,
        out_shape=out_shape,
        scratch_shapes=scratch,
        input_output_aliases=aliases or {},
        name=name,
        cost_estimate=pl.CostEstimate(flops=int(flops), bytes_accessed=int(moved), transcendentals=0),
        compiler_params=pltpu.CompilerParams(**params),
    )
    return run if gather is None else lambda *operands: run(*operands, *sources)


MESH = pl.DeviceIdType.MESH
ANY = pl.BlockSpec(memory_space=pl.ANY)
UNITS = 4


class Gather:
    def __init__(self, pieces, group):
        self.pieces, self.group = pieces, group
        self.count = len(pieces)

    def out_shape(self, rows, width):
        return [jax.ShapeDtypeStruct((self.group * rows, width), BF16)] * self.count

    def scratch(self):
        return [pltpu.SemaphoreType.DMA((self.count, 16)), pltpu.SemaphoreType.DMA((self.count, 16))] if self.count else []

    def bind(self, sources, outs, sems):
        self.sources, self.outs = sources, outs
        self.send, self.recv = sems
        me, n = lax.axis_index("dp"), self.group
        rep = lax.axis_index("rep")
        self.core = lax.rem(rep, 2)
        self.me, self.right, self.left = me, lax.rem(me + 1, n), lax.rem(me + n - 1, n)
        self.to_right, self.to_left = {"dp": self.right}, {"dp": self.left}
        self.to_other = {"rep": rep + 1 - 2 * self.core}

    def source(self, k, unit):
        which, layer, chunk, tall = self.pieces[k]
        ref, out = self.sources[which], self.outs[k]
        rows, width = out.shape[0] // self.group, out.shape[1] // UNITS
        if tall:
            return ref.at[layer, pl.ds(chunk * rows, rows), pl.ds(pl.multiple_of(unit * width, width), width)]
        return ref.at[layer, :, pl.ds(pl.multiple_of((unit * CHUNKS + chunk) * width, width), width)]

    def place(self, k, owner, unit):
        out = self.outs[k]
        rows, width = out.shape[0] // self.group, out.shape[1] // UNITS
        return out.at[pl.ds(pl.multiple_of(owner * rows, rows), rows), pl.ds(pl.multiple_of(unit * width, width), width)]

    def copy(self, k, slot, source, target, device):
        return pltpu.make_async_remote_copy(
            src_ref=source, dst_ref=target, send_sem=self.send.at[k, slot], recv_sem=self.recv.at[k, slot], device_id=device, device_id_type=MESH
        )

    def own(self, k):
        return [self.copy(k, u, self.source(k, u), self.place(k, self.me, u), self.to_other) for u in range(UNITS)]

    def near(self, k):
        sends = []
        for u in range(2):
            unit = 2 * self.core + u
            sends.append(self.copy(k, 4 + u, self.source(k, unit), self.place(k, self.me, unit), self.to_right))
            sends.append(self.copy(k, 6 + u, self.source(k, unit), self.place(k, self.me, unit), self.to_left))
        return sends

    def on(self, k):
        first, second = 2 * self.core, 2 * self.core + 1
        from_left, from_right = self.place(k, self.left, first), self.place(k, self.right, second)
        return [self.copy(k, 12, from_left, from_left, self.to_right), self.copy(k, 13, from_right, from_right, self.to_left)]

    def across(self, k):
        sends = []
        for u in range(2):
            for slot, owner in ((8, self.left), (10, self.right)):
                block = self.place(k, owner, 2 * self.core + u)
                sends.append(self.copy(k, slot + u, block, block, self.to_other))
        return sends

    def across_far(self, k):
        far = lax.rem(self.me + 2, self.group)
        return [self.copy(k, 14 + u, b, b, self.to_other) for u in range(2) for b in [self.place(k, far, 2 * self.core + u)]]

    def begin(self):
        barrier = pltpu.get_barrier_semaphore()
        for device in (self.to_right, self.to_left, self.to_other):
            pl.semaphore_signal(barrier, inc=1, device_id=device, device_id_type=MESH)
        pl.semaphore_wait(barrier, 3)
        for k in range(self.count):
            for copy in self.near(k):
                copy.start()
        for k in range(self.count):
            for copy in self.own(k):
                copy.start()

    def pass_on(self):
        for k in range(self.count):
            for copy in self.near(k):
                copy.wait_recv()
            for copy in self.on(k):
                copy.start()
            for copy in self.across(k):
                copy.start()

    def pass_far(self):
        for k in range(self.count):
            for copy in self.on(k):
                copy.wait_recv()
            for copy in self.across_far(k):
                copy.start()

    def end(self):
        for k in range(self.count):
            for copies in (self.own(k), self.across(k), self.across_far(k)):
                for copy in copies:
                    copy.wait_recv()
            for copies in (self.own(k), self.near(k), self.on(k), self.across(k), self.across_far(k)):
                for copy in copies:
                    copy.wait_send()


def once(shape, index):
    return pl.BlockSpec(shape, index, pipeline_mode=pl.Buffered(1))


def nothing_kernel():
    pass


def fetch(gather, ident, sources):
    return call(nothing_kernel, (1,), [], [], [], 10**9, 10**7, name="fetch", gather=gather, when=(1, 1), ident=ident, sources=sources)()


def gate_up_kernel(first, h, wg, wu, *refs):
    if first:
        a_out, p, gate, up, a = refs
        wide = h[...].astype(F32)
        a[...] = (wide * norm_scale(wide)).astype(BF16)
        a_out[...] = a[...]
    else:
        p, gate, up = refs
        a = h
    half = wg.shape[1] // 2
    for part in range(2):
        cols = pl.ds(part * half, half)
        g = dot(a[...], wg[:, cols], 1, 0)
        u = dot(a[...], wu[:, cols], 1, 0)
        gate[:, cols] = g
        up[:, cols] = u
        p[:, cols] = (g * jax.nn.sigmoid(g) * u).astype(BF16)


def gate_up(first, h, wg, wu, **extra):
    t, d = h.shape
    f = wg.shape[1]
    tm = min(t, 512)
    token = pl.BlockSpec((tm, d), lambda i: (i, 0))
    tile = pl.BlockSpec((tm, f), lambda i: (i, 0))
    whole = once((d, f), lambda i: (0, 0))
    return call(
        functools.partial(gate_up_kernel, first),
        (t // tm,),
        [token, whole, whole],
        [token] * first + [tile, tile, tile],
        [jax.ShapeDtypeStruct((t, d), BF16)] * first + [jax.ShapeDtypeStruct((t, f), BF16)] + [jax.ShapeDtypeStruct((t, f), F32)] * 2,
        4 * t * d * f,
        10 * t * f,
        [pltpu.VMEM((tm, d), BF16)] * first,
        name="gate_up",
        **extra,
    )(h, wg, wu)


def down_kernel(pieces, h, *refs):
    ps, ws, (h_out, a_out) = refs[:pieces], refs[pieces : 2 * pieces], refs[2 * pieces :]
    total = dot(ps[0][...], ws[0][...], 1, 0)
    for p, w in zip(ps[1:], ws[1:]):
        total = total + dot(p[...], w[...], 1, 0)
    new = (h[...].astype(F32) + rounded(total)).astype(BF16)
    h_out[...] = new
    wide = new.astype(F32)
    a_out[...] = (wide * norm_scale(wide)).astype(BF16)


def down(ps, ws, h, **extra):
    t, d = h.shape
    n, f = len(ps), ps[0].shape[1]
    tm = min(t, 512)
    token = pl.BlockSpec((tm, d), lambda i: (i, 0))
    return call(
        functools.partial(down_kernel, n),
        (t // tm,),
        [token] + [pl.BlockSpec((tm, f), lambda i: (i, 0))] * n + [once((f, d), lambda i: (0, 0))] * n,
        [token, token],
        [jax.ShapeDtypeStruct((t, d), BF16)] * 2,
        2 * t * d * f * n,
        2 * t * f * n,
        name="down",
        **extra,
    )(h, *ps, *ws)


def hidden_gradients(g, u, dp):
    s = jax.nn.sigmoid(g)
    silu = g * s
    return silu, dp * u * (s * (1 + g * (1 - s))), dp * silu


def hidden_kernel(a, dy, wg, wu, wd, p, dg, du):
    half = wg.shape[1] // 2
    for part in range(2):
        cols = pl.ds(part * half, half)
        g = dot(a[...], wg[:, cols], 1, 0)
        u = dot(a[...], wu[:, cols], 1, 0)
        dp = rounded(dot(dy[...], wd[cols, :], 1, 1))
        silu, by_g, by_u = hidden_gradients(g, u, dp)
        p[:, cols] = (silu * u).astype(BF16)
        dg[:, cols] = by_g.astype(BF16)
        du[:, cols] = by_u.astype(BF16)


def hidden(a, dy, wg, wu, wd, **extra):
    t, d = a.shape
    f = wg.shape[1]
    tm = min(t, 1024 if extra.get("gather") is None else 512)
    token = pl.BlockSpec((tm, d), lambda i: (i, 0))
    tile = pl.BlockSpec((tm, f), lambda i: (i, 0))
    whole = lambda shape: once(shape, lambda i: (0, 0))
    return call(
        hidden_kernel,
        (t // tm,),
        [token, token, whole((d, f)), whole((d, f)), whole((f, d))],
        [tile] * 3,
        [jax.ShapeDtypeStruct((t, f), BF16)] * 3,
        6 * t * d * f,
        6 * t * f,
        name="hidden",
        **extra,
    )(a, dy, wg, wu, wd)


def hidden_back_kernel(dh, wd, gate, up, dg, du):
    half = wd.shape[0] // 2
    for part in range(2):
        cols = pl.ds(part * half, half)
        dp = rounded(dot(dh[...], wd[cols, :], 1, 1))
        _, by_g, by_u = hidden_gradients(gate[:, cols], up[:, cols], dp)
        dg[:, cols] = by_g.astype(BF16)
        du[:, cols] = by_u.astype(BF16)


def hidden_back(dh, wd, gate, up):
    t, d = dh.shape
    f = wd.shape[0]
    tm = min(t, 512)
    token = pl.BlockSpec((tm, d), lambda i: (i, 0))
    tile = pl.BlockSpec((tm, f), lambda i: (i, 0))
    return call(
        hidden_back_kernel,
        (t // tm,),
        [token, once((f, d), lambda i: (0, 0)), tile, tile],
        [tile] * 2,
        [jax.ShapeDtypeStruct((t, f), BF16)] * 2,
        2 * t * d * f,
        12 * t * f,
        name="hidden_back",
    )(dh, wd, gate, up)


def by_weights_kernel(n, halves, dy, a, *refs):
    ps, dgs, dus = (refs[k * n : k * n + n] for k in range(3))
    out, acc_d, acc_g, acc_u = refs[3 * n :]
    chunk, i = pl.program_id(0) // halves, pl.program_id(1)
    half = lax.rem(pl.program_id(0), halves)
    group, rows = out.shape[0], out.shape[3]
    for c in range(n):

        @pl.when(chunk == c)
        def _():
            terms = dot(ps[c][...], dy[...], 0, 0), dot(a[...], dgs[c][...], 0, 0), dot(a[...], dus[c][...], 0, 0)

            @pl.when(i == 0)
            def _():
                for acc, term in zip((acc_d, acc_g, acc_u), terms):
                    acc[...] = term

            @pl.when(i > 0)
            def _():
                by_d, by_g, by_u = ((acc[...] + term).astype(BF16) for acc, term in zip((acc_d, acc_g, acc_u), terms))
                part = group // halves
                out[pl.ds(half * part, part), 0, 0] = by_d.reshape(part, rows, by_d.shape[1])
                width = by_g.shape[1]
                for h in range(halves):

                    @pl.when(half == h)
                    def _():
                        out[:, 0, 1, :, pl.ds(h * width, width)] = by_g.reshape(group, rows, width)
                        out[:, 0, 2, :, pl.ds(h * width, width)] = by_u.reshape(group, rows, width)


def by_weights(ps, dgs, dus, dy, a, group):
    t, d = a.shape
    n, f = len(ps), ps[0].shape[1]
    halves, steps = 2, 2
    tm, width = t // steps, f // halves
    token = pl.BlockSpec((tm, d), lambda j, i: (i, 0))

    def tile(c):
        def index(j, i):
            before, after = j < c * halves, j >= (c + 1) * halves
            row = jnp.where(before, 0, jnp.where(after, steps - 1, i))
            return row, jnp.where(before, 0, jnp.where(after, halves - 1, j - c * halves))

        return pl.BlockSpec((tm, width), index if n > 1 else lambda j, i: (i, j))

    return call(
        functools.partial(by_weights_kernel, n, halves),
        (n * halves, steps),
        [token, token] + [tile(c) for c in range(n)] * 3,
        pl.BlockSpec((group, 1, 3, d // group, f), lambda j, i: (0, j // halves, 0, 0, 0)),
        jax.ShapeDtypeStruct((group, n, 3, d // group, f), BF16),
        6 * t * d * f * n,
        10 * t * f * n,
        [pltpu.VMEM((width, d), F32)] + [pltpu.VMEM((d, width), F32)] * 2,
        name="by_weights",
    )(dy, a, *ps, *dgs, *dus)


def by_input_kernel(n, h, dy, *refs):
    dgs, dus, wgs, wus = (refs[k * n : k * n + n] for k in range(4))
    out = refs[4 * n]

    def back(parts, ws):
        total = dot(parts[0][...], ws[0][...], 1, 1)
        for part, w in zip(parts[1:], ws[1:]):
            total = total + dot(part[...], w[...], 1, 1)
        return rounded(total)

    da = rounded(back(dgs, wgs) + back(dus, wus))
    wide = h[...].astype(F32)
    scale = norm_scale(wide)
    by_scale = jnp.sum(da * wide, -1, keepdims=True)
    by_wide = da * scale - (by_scale * scale * scale * scale / wide.shape[-1]) * wide
    out[...] = (dy[...].astype(F32) + rounded(by_wide)).astype(BF16)


def by_input(h, dy, dgs, dus, wgs, wus):
    t, d = h.shape
    n, f = len(dgs), dgs[0].shape[1]
    tm = min(t, 512)
    token = pl.BlockSpec((tm, d), lambda i: (i, 0))
    return call(
        functools.partial(by_input_kernel, n),
        (t // tm,),
        [token, token] + [pl.BlockSpec((tm, f), lambda i: (i, 0))] * (2 * n) + [once((d, f), lambda i: (0, 0))] * (2 * n),
        token,
        jax.ShapeDtypeStruct((t, d), BF16),
        4 * t * d * n * f,
        4 * t * n * f,
        name="by_input",
    )(h, dy, *dgs, *dus, *wgs, *wus)


def adamw_kernel(had, *refs):
    grads, refs = refs[:3], refs[3:]
    old, new = refs[:9], refs[9 + had :]
    for k in range(3):
        g = grads[k][0, 0].astype(F32)
        w, m, v = (old[k + 3 * which][0] for which in range(3))
        m = 0.9 * m + 0.1 * g
        v = 0.95 * v + 0.05 * g * g
        w = w.astype(F32)
        new[k][0] = (w - 0.02 * (m * lax.rsqrt(v + 1e-8) + 0.1 * w)).astype(BF16)
        new[k + 3][0] = m
        new[k + 6][0] = v


def adamw(grads, arrays, so_far, layer, start, group):
    n, _, rows, width = grads.shape
    part = width // group
    wide = pl.BlockSpec((1, rows, part), lambda c, i: (layer, 0, CHUNKS * i + c + start))
    tall = pl.BlockSpec((1, rows // group, width), lambda c, i: (layer, group * (c + start) + i, 0))
    blocks = [wide, wide, tall] * 3
    sums = [
        pl.BlockSpec((1, 1, rows, part), lambda c, i: (c, 1, 0, i)),
        pl.BlockSpec((1, 1, rows, part), lambda c, i: (c, 2, 0, i)),
        pl.BlockSpec((1, 1, rows // group, width), lambda c, i: (c, 0, i, 0)),
    ]
    had = len(so_far)
    return call(
        functools.partial(adamw_kernel, had),
        (n, group),
        sums + blocks + [pl.BlockSpec(memory_space=pl.ANY)] * had,
        blocks,
        [jax.ShapeDtypeStruct(a.shape, a.dtype) for a in arrays],
        20 * grads.size,
        22 * grads.size,
        aliases={3 + len(arrays) + k: k for k in range(had)},
        name="adamw",
    )(grads, grads, grads, *arrays, *so_far)


def solution(mesh):
    group = mesh.shape["dp"]

    def step(x, dy, *arrays):
        weights = arrays[:3]
        layers, rows, width = weights[0].shape
        h0, dy = x[0], dy[0]

        def summed(grads):
            _, n, _, rows, width = grads.shape
            mine = lax.psum_scatter(grads.reshape(group * n * 3 * rows, width), "dp", scatter_dimension=0, tiled=True)
            return mine.reshape(n, 3, rows, width)

        ident = iter(range(100))

        def beside(*pieces, when):
            gather = Gather([(which, layer, chunk, which == 2) for which, layer, chunk in pieces], group)
            return dict(gather=gather, when=when, ident=next(ident), sources=weights)

        wg, wu, wd = ([[None] * CHUNKS for _ in range(layers)] for _ in range(3))

        def keep(got, *pieces):
            for array, (which, layer, chunk) in zip(got, pieces, strict=True):
                (wg, wu, wd)[which][layer][chunk] = array

        pieces = (0, 0, 0), (1, 0, 0)
        extra = beside(*pieces, when=(1, 1))
        keep(fetch(extra["gather"], extra["ident"], weights), *pieces)
        plan = [
            [(0, 0, 1), (1, 0, 1)],
            [(0, 0, 2), (1, 0, 2), (2, 0, 0)],
            [(0, 0, 3), (1, 0, 3), (2, 0, 1)],
            [(2, 0, 2), (2, 0, 3)],
        ]
        ps, gates, ups, a0 = [], [], [], None
        for c in range(CHUNKS):
            got = gate_up(c == 0, h0 if c == 0 else a0, wg[0][c], wu[0][c], **beside(*plan[c], when=(5, 8)))
            if c == 0:
                a0, *got = got
            p, gate, up, *got = got
            keep(got, *plan[c])
            ps.append(p)
            gates.append(gate)
            ups.append(up)
        pieces = [(which, 1, 0) for which in range(3)]
        h1, a1, *got = down(ps, wd[0], h0, **beside(*pieces, when=(4, 6)))
        keep(got, *pieces)
        sums, qs, dgs, dus = [], [], [], []
        for c in range(CHUNKS):
            pieces = [(which, 1, c + 1) for which in range(3)] if c + 1 < CHUNKS else []
            q, dg, du, *got = hidden(a1, dy, wg[1][c], wu[1][c], wd[1][c], **(beside(*pieces, when=(5, 8)) if pieces else {}))
            keep(got, *pieces)
            qs.append(q)
            dgs.append(dg)
            dus.append(du)
            for start, stop in LAST_RANGES:
                if stop == c + 1:
                    sums.append((1, start, summed(by_weights(qs[start:stop], dgs[start:stop], dus[start:stop], dy, a1, group))))
        dh = by_input(h1, dy, dgs, dus, wg[1], wu[1])
        for c in range(CHUNKS):
            dg, du = hidden_back(dh, wd[0][c], gates[c], ups[c])
            sums.append((0, c, summed(by_weights([ps[c]], [dg], [du], dh, a0, group))))
        new = ()
        for layer, start, grads in sums:
            new = adamw(grads, arrays, new, layer, start, group)
        return tuple(new)

    states, cut = P(("rep", "dp"), None, None), P(None, "dp", None)
    return jax.shard_map(
        step,
        mesh=mesh,
        in_specs=(states, states) + (cut,) * 9,
        out_specs=(P("rep", "dp", None),) * 9,
        check_vma=False,
    )
```

```python
import functools

import jax
import jax.numpy as jnp
from jax import lax
from jax.experimental import pallas as pl
from jax.experimental.pallas import tpu as pltpu
from jax.sharding import PartitionSpec as P

F32, BF16 = jnp.float32, jnp.bfloat16
VMEM_LIMIT = 61 * 2**20
CHUNKS = 4


def dot(a, b, over_a, over_b):
    return lax.dot_general(a, b, (((over_a,), (over_b,)), ((), ())), preferred_element_type=F32)


def rounded(a):
    return a.astype(BF16).astype(F32)


def norm_scale(wide):
    return lax.rsqrt(jnp.mean(wide * wide, -1, keepdims=True) + 1e-6)


def riding(kernel, ins, outs, gather, steps, when):
    def whole(*refs):
        refs = list(refs)
        take = lambda n: [refs.pop(0) for _ in range(n)]
        mine, sources, results, gathered = take(ins), take(3), take(outs), take(gather.count)
        sems = [refs.pop(), refs.pop()]
        gather.bind(sources, gathered, sems[::-1])
        index = 0
        for axis in range(len(steps)):
            index = index * steps[axis] + pl.program_id(axis)
        total = 1
        for n in steps:
            total *= n
        pl.when(index == 0)(gather.begin)
        if when[0] < total:
            pl.when(index == when[0])(gather.pass_on)
        if when[1] < total:
            pl.when(index == when[1])(gather.pass_far)
        kernel(*mine, *results, *refs)

        @pl.when(index == total - 1)
        def _():
            if when[0] >= total:
                gather.pass_on()
            if when[1] >= total:
                gather.pass_far()
            gather.end()

    return whole


def call(kernel, grid, in_specs, out_specs, out_shape, flops, moved, scratch=(), aliases=None, name=None, gather=None, when=None, ident=None, sources=None):
    params = dict(vmem_limit_bytes=VMEM_LIMIT)
    in_specs, out_specs, out_shape, scratch = list(in_specs), out_specs, out_shape, list(scratch)
    if gather is not None:
        kernel = riding(kernel, len(in_specs), len(out_specs), gather, grid, when)
        in_specs = in_specs + [ANY] * 3
        out_specs = list(out_specs) + [ANY] * gather.count
        out_shape = list(out_shape) + gather.out_shape(sources[0].shape[1], sources[2].shape[2])
        scratch = scratch + gather.scratch()
        params.update(collective_id=ident, has_side_effects=True)
    run = pl.pallas_call(
        kernel,
        grid=grid,
        in_specs=in_specs,
        out_specs=out_specs,
        out_shape=out_shape,
        scratch_shapes=scratch,
        input_output_aliases=aliases or {},
        name=name,
        cost_estimate=pl.CostEstimate(flops=int(flops), bytes_accessed=int(moved), transcendentals=0),
        compiler_params=pltpu.CompilerParams(**params),
    )
    return run if gather is None else lambda *operands: run(*operands, *sources)


MESH = pl.DeviceIdType.MESH
ANY = pl.BlockSpec(memory_space=pl.ANY)
UNITS = 4


class Gather:
    def __init__(self, pieces, group):
        self.pieces, self.group = pieces, group
        self.count = len(pieces)

    def out_shape(self, rows, width):
        return [jax.ShapeDtypeStruct((self.group * rows, width), BF16)] * self.count

    def scratch(self):
        return [pltpu.SemaphoreType.DMA((self.count, 16)), pltpu.SemaphoreType.DMA((self.count, 16))] if self.count else []

    def bind(self, sources, outs, sems):
        self.sources, self.outs = sources, outs
        self.send, self.recv = sems
        me, n = lax.axis_index("dp"), self.group
        rep = lax.axis_index("rep")
        self.core = lax.rem(rep, 2)
        self.me, self.right, self.left = me, lax.rem(me + 1, n), lax.rem(me + n - 1, n)
        self.to_right, self.to_left = {"dp": self.right}, {"dp": self.left}
        self.to_other = {"rep": rep + 1 - 2 * self.core}

    def source(self, k, unit):
        which, layer, chunk, tall = self.pieces[k]
        ref, out = self.sources[which], self.outs[k]
        rows, width = out.shape[0] // self.group, out.shape[1] // UNITS
        if tall:
            return ref.at[layer, pl.ds(chunk * rows, rows), pl.ds(pl.multiple_of(unit * width, width), width)]
        return ref.at[layer, :, pl.ds(pl.multiple_of((unit * CHUNKS + chunk) * width, width), width)]

    def place(self, k, owner, unit):
        out = self.outs[k]
        rows, width = out.shape[0] // self.group, out.shape[1] // UNITS
        return out.at[pl.ds(pl.multiple_of(owner * rows, rows), rows), pl.ds(pl.multiple_of(unit * width, width), width)]

    def copy(self, k, slot, source, target, device):
        return pltpu.make_async_remote_copy(
            src_ref=source, dst_ref=target, send_sem=self.send.at[k, slot], recv_sem=self.recv.at[k, slot], device_id=device, device_id_type=MESH
        )

    def own(self, k):
        return [self.copy(k, u, self.source(k, u), self.place(k, self.me, u), self.to_other) for u in range(UNITS)]

    def near(self, k):
        sends = []
        for u in range(2):
            unit = 2 * self.core + u
            sends.append(self.copy(k, 4 + u, self.source(k, unit), self.place(k, self.me, unit), self.to_right))
            sends.append(self.copy(k, 6 + u, self.source(k, unit), self.place(k, self.me, unit), self.to_left))
        return sends

    def on(self, k):
        first, second = 2 * self.core, 2 * self.core + 1
        from_left, from_right = self.place(k, self.left, first), self.place(k, self.right, second)
        return [self.copy(k, 12, from_left, from_left, self.to_right), self.copy(k, 13, from_right, from_right, self.to_left)]

    def across(self, k):
        sends = []
        for u in range(2):
            for slot, owner in ((8, self.left), (10, self.right)):
                block = self.place(k, owner, 2 * self.core + u)
                sends.append(self.copy(k, slot + u, block, block, self.to_other))
        return sends

    def across_far(self, k):
        far = lax.rem(self.me + 2, self.group)
        return [self.copy(k, 14 + u, b, b, self.to_other) for u in range(2) for b in [self.place(k, far, 2 * self.core + u)]]

    def begin(self):
        barrier = pltpu.get_barrier_semaphore()
        for device in (self.to_right, self.to_left, self.to_other):
            pl.semaphore_signal(barrier, inc=1, device_id=device, device_id_type=MESH)
        pl.semaphore_wait(barrier, 3)
        for k in range(self.count):
            for copy in self.near(k):
                copy.start()
        for k in range(self.count):
            for copy in self.own(k):
                copy.start()

    def pass_on(self):
        for k in range(self.count):
            for copy in self.near(k):
                copy.wait_recv()
            for copy in self.on(k):
                copy.start()
            for copy in self.across(k):
                copy.start()

    def pass_far(self):
        for k in range(self.count):
            for copy in self.on(k):
                copy.wait_recv()
            for copy in self.across_far(k):
                copy.start()

    def end(self):
        for k in range(self.count):
            for copies in (self.own(k), self.across(k), self.across_far(k)):
                for copy in copies:
                    copy.wait_recv()
            for copies in (self.own(k), self.near(k), self.on(k), self.across(k), self.across_far(k)):
                for copy in copies:
                    copy.wait_send()


def once(shape, index):
    return pl.BlockSpec(shape, index, pipeline_mode=pl.Buffered(1))


def nothing_kernel():
    pass


def fetch(gather, ident, sources):
    return call(nothing_kernel, (1,), [], [], [], 10**9, 10**7, name="fetch", gather=gather, when=(1, 1), ident=ident, sources=sources)()


def gate_up_kernel(first, h, wg, wu, *refs):
    if first:
        a_out, p, gate, up, a = refs
        wide = h[...].astype(F32)
        a[...] = (wide * norm_scale(wide)).astype(BF16)
        a_out[...] = a[...]
    else:
        p, gate, up = refs
        a = h
    half = wg.shape[1] // 2
    for part in range(2):
        cols = pl.ds(part * half, half)
        g = dot(a[...], wg[:, cols], 1, 0)
        u = dot(a[...], wu[:, cols], 1, 0)
        gate[:, cols] = g
        up[:, cols] = u
        p[:, cols] = (g * jax.nn.sigmoid(g) * u).astype(BF16)


def gate_up(first, h, wg, wu, **extra):
    t, d = h.shape
    f = wg.shape[1]
    tm = min(t, 512)
    token = pl.BlockSpec((tm, d), lambda i: (i, 0))
    tile = pl.BlockSpec((tm, f), lambda i: (i, 0))
    whole = once((d, f), lambda i: (0, 0))
    return call(
        functools.partial(gate_up_kernel, first),
        (t // tm,),
        [token, whole, whole],
        [token] * first + [tile, tile, tile],
        [jax.ShapeDtypeStruct((t, d), BF16)] * first + [jax.ShapeDtypeStruct((t, f), BF16)] + [jax.ShapeDtypeStruct((t, f), F32)] * 2,
        4 * t * d * f,
        10 * t * f,
        [pltpu.VMEM((tm, d), BF16)] * first,
        name="gate_up",
        **extra,
    )(h, wg, wu)


def down_kernel(pieces, h, *refs):
    ps, ws, (h_out, a_out) = refs[:pieces], refs[pieces : 2 * pieces], refs[2 * pieces :]
    total = dot(ps[0][...], ws[0][...], 1, 0)
    for p, w in zip(ps[1:], ws[1:]):
        total = total + dot(p[...], w[...], 1, 0)
    new = (h[...].astype(F32) + rounded(total)).astype(BF16)
    h_out[...] = new
    wide = new.astype(F32)
    a_out[...] = (wide * norm_scale(wide)).astype(BF16)


def down(ps, ws, h, **extra):
    t, d = h.shape
    n, f = len(ps), ps[0].shape[1]
    tm = min(t, 512)
    token = pl.BlockSpec((tm, d), lambda i: (i, 0))
    return call(
        functools.partial(down_kernel, n),
        (t // tm,),
        [token] + [pl.BlockSpec((tm, f), lambda i: (i, 0))] * n + [once((f, d), lambda i: (0, 0))] * n,
        [token, token],
        [jax.ShapeDtypeStruct((t, d), BF16)] * 2,
        2 * t * d * f * n,
        2 * t * f * n,
        name="down",
        **extra,
    )(h, *ps, *ws)


def hidden_gradients(g, u, dp):
    s = jax.nn.sigmoid(g)
    silu = g * s
    return silu, dp * u * (s * (1 + g * (1 - s))), dp * silu


def hidden_kernel(a, dy, wg, wu, wd, p, dg, du):
    half = wg.shape[1] // 2
    for part in range(2):
        cols = pl.ds(part * half, half)
        g = dot(a[...], wg[:, cols], 1, 0)
        u = dot(a[...], wu[:, cols], 1, 0)
        dp = rounded(dot(dy[...], wd[cols, :], 1, 1))
        silu, by_g, by_u = hidden_gradients(g, u, dp)
        p[:, cols] = (silu * u).astype(BF16)
        dg[:, cols] = by_g.astype(BF16)
        du[:, cols] = by_u.astype(BF16)


def hidden(a, dy, wg, wu, wd, **extra):
    t, d = a.shape
    f = wg.shape[1]
    tm = min(t, 1024 if extra.get("gather") is None else 512)
    token = pl.BlockSpec((tm, d), lambda i: (i, 0))
    tile = pl.BlockSpec((tm, f), lambda i: (i, 0))
    whole = lambda shape: once(shape, lambda i: (0, 0))
    return call(
        hidden_kernel,
        (t // tm,),
        [token, token, whole((d, f)), whole((d, f)), whole((f, d))],
        [tile] * 3,
        [jax.ShapeDtypeStruct((t, f), BF16)] * 3,
        6 * t * d * f,
        6 * t * f,
        name="hidden",
        **extra,
    )(a, dy, wg, wu, wd)


def first_kernel(dh, a, wd, gate, up, p, out, dg, du, acc_d, acc_g, acc_u):
    i, last = pl.program_id(1), pl.num_programs(1) - 1
    width = wd.shape[0]
    half = width // 2
    for part in range(2):
        cols = pl.ds(part * half, half)
        dp = rounded(dot(dh[...], wd[cols, :], 1, 1))
        _, by_g, by_u = hidden_gradients(gate[:, cols], up[:, cols], dp)
        dg[:, cols] = by_g.astype(BF16)
        du[:, cols] = by_u.astype(BF16)
    terms = dot(p[...], dh[...], 0, 0), dot(a[...], dg[...], 0, 0), dot(a[...], du[...], 0, 0)
    accs = acc_d, acc_g, acc_u

    @pl.when(i == 0)
    def _():
        for acc, term in zip(accs, terms):
            acc[...] = term

    @pl.when(i > 0)
    def _():
        for acc, term in zip(accs, terms):
            acc[...] += term

    group, rows = out.shape[0], out.shape[3]
    halves = out.shape[4] // width
    part = group // halves
    for h in range(halves):

        @pl.when((i == last) & (pl.program_id(0) == h))
        def _():
            out[h * part : (h + 1) * part, 0, 0] = acc_d[...].astype(BF16).reshape(part, rows, out.shape[4])
            out[:, 0, 1, :, h * width : (h + 1) * width] = acc_g[...].astype(BF16).reshape(group, rows, width)
            out[:, 0, 2, :, h * width : (h + 1) * width] = acc_u[...].astype(BF16).reshape(group, rows, width)


def first_back(dh, a, wd, gate, up, p, group):
    t, d = a.shape
    f = wd.shape[0]
    halves, tm = 2, min(t, 1024)
    width = f // halves
    token = pl.BlockSpec((tm, d), lambda j, i: (i, 0))
    tile = pl.BlockSpec((tm, width), lambda j, i: (i, j))
    return call(
        first_kernel,
        (halves, t // tm),
        [token, token, pl.BlockSpec((width, d), lambda j, i: (j, 0)), tile, tile, tile],
        pl.BlockSpec((group, 1, 3, d // group, f), lambda j, i: (0, 0, 0, 0, 0)),
        jax.ShapeDtypeStruct((group, 1, 3, d // group, f), BF16),
        8 * t * d * f,
        10 * t * f,
        [pltpu.VMEM((tm, width), BF16)] * 2 + [pltpu.VMEM((width, d), F32)] + [pltpu.VMEM((d, width), F32)] * 2,
        name="first_back",
    )(dh, a, wd, gate, up, p)


def by_weights_kernel(n, halves, dy, a, *refs):
    ps, dgs, dus = (refs[k * n : k * n + n] for k in range(3))
    _, out, acc_d, acc_g, acc_u = refs[3 * n :]
    chunk, i = pl.program_id(0) // halves, pl.program_id(1)
    half = lax.rem(pl.program_id(0), halves)
    group, rows = out.shape[0], out.shape[3]
    for c in range(n):

        @pl.when(chunk == c)
        def _():
            terms = dot(ps[c][...], dy[...], 0, 0), dot(a[...], dgs[c][...], 0, 0), dot(a[...], dus[c][...], 0, 0)

            @pl.when(i == 0)
            def _():
                for acc, term in zip((acc_d, acc_g, acc_u), terms):
                    acc[...] = term

            @pl.when(i > 0)
            def _():
                by_d, by_g, by_u = ((acc[...] + term).astype(BF16) for acc, term in zip((acc_d, acc_g, acc_u), terms))
                part = group // halves
                out[pl.ds(half * part, part), 0, 0] = by_d.reshape(part, rows, by_d.shape[1])
                width = by_g.shape[1]
                for h in range(halves):

                    @pl.when(half == h)
                    def _():
                        out[:, 0, 1, :, pl.ds(h * width, width)] = by_g.reshape(group, rows, width)
                        out[:, 0, 2, :, pl.ds(h * width, width)] = by_u.reshape(group, rows, width)


def by_weights(ps, dgs, dus, dy, a, group, after):
    t, d = a.shape
    n, f = len(ps), ps[0].shape[1]
    halves, steps = 2, 2
    tm, width = t // steps, f // halves
    token = pl.BlockSpec((tm, d), lambda j, i: (i, 0))

    def tile(c):
        def index(j, i):
            before, after = j < c * halves, j >= (c + 1) * halves
            row = jnp.where(before, 0, jnp.where(after, steps - 1, i))
            return row, jnp.where(before, 0, jnp.where(after, halves - 1, j - c * halves))

        return pl.BlockSpec((tm, width), index if n > 1 else lambda j, i: (i, j))

    return call(
        functools.partial(by_weights_kernel, n, halves),
        (n * halves, steps),
        [token, token] + [tile(c) for c in range(n)] * 3 + [ANY],
        pl.BlockSpec((group, 1, 3, d // group, f), lambda j, i: (0, j // halves, 0, 0, 0)),
        jax.ShapeDtypeStruct((group, n, 3, d // group, f), BF16),
        6 * t * d * f * n,
        10 * t * f * n,
        [pltpu.VMEM((width, d), F32)] + [pltpu.VMEM((d, width), F32)] * 2,
        name="by_weights",
    )(dy, a, *ps, *dgs, *dus, after)


def by_input_kernel(n, h, dy, *refs):
    dgs, dus, wgs, wus = (refs[k * n : k * n + n] for k in range(4))
    out = refs[4 * n]

    def back(parts, ws):
        total = dot(parts[0][...], ws[0][...], 1, 1)
        for part, w in zip(parts[1:], ws[1:]):
            total = total + dot(part[...], w[...], 1, 1)
        return rounded(total)

    da = rounded(back(dgs, wgs) + back(dus, wus))
    wide = h[...].astype(F32)
    scale = norm_scale(wide)
    by_scale = jnp.sum(da * wide, -1, keepdims=True)
    by_wide = da * scale - (by_scale * scale * scale * scale / wide.shape[-1]) * wide
    out[...] = (dy[...].astype(F32) + rounded(by_wide)).astype(BF16)


def by_input(h, dy, dgs, dus, wgs, wus):
    t, d = h.shape
    n, f = len(dgs), dgs[0].shape[1]
    tm = min(t, 512)
    token = pl.BlockSpec((tm, d), lambda i: (i, 0))
    return call(
        functools.partial(by_input_kernel, n),
        (t // tm,),
        [token, token] + [pl.BlockSpec((tm, f), lambda i: (i, 0))] * (2 * n) + [once((d, f), lambda i: (0, 0))] * (2 * n),
        token,
        jax.ShapeDtypeStruct((t, d), BF16),
        4 * t * d * n * f,
        4 * t * n * f,
        name="by_input",
    )(h, dy, *dgs, *dus, *wgs, *wus)


def adamw_kernel(had, *refs):
    grads, refs = refs[:3], refs[3:]
    old, new = refs[:9], refs[9 + had :]
    for k in range(3):
        g = grads[k][0, 0].astype(F32)
        w, m, v = (old[k + 3 * which][0] for which in range(3))
        m = 0.9 * m + 0.1 * g
        v = 0.95 * v + 0.05 * g * g
        w = w.astype(F32)
        new[k][0] = (w - 0.02 * (m * lax.rsqrt(v + 1e-8) + 0.1 * w)).astype(BF16)
        new[k + 3][0] = m
        new[k + 6][0] = v


def adamw(grads, arrays, so_far, layer, start, group):
    n, _, rows, width = grads.shape
    part = width // group
    wide = pl.BlockSpec((1, rows, part), lambda c, i: (layer, 0, CHUNKS * i + c + start))
    tall = pl.BlockSpec((1, rows // group, width), lambda c, i: (layer, group * (c + start) + i, 0))
    blocks = [wide, wide, tall] * 3
    sums = [
        pl.BlockSpec((1, 1, rows, part), lambda c, i: (c, 1, 0, i)),
        pl.BlockSpec((1, 1, rows, part), lambda c, i: (c, 2, 0, i)),
        pl.BlockSpec((1, 1, rows // group, width), lambda c, i: (c, 0, i, 0)),
    ]
    had = len(so_far)
    return call(
        functools.partial(adamw_kernel, had),
        (n, group),
        sums + blocks + [pl.BlockSpec(memory_space=pl.ANY)] * had,
        blocks,
        [jax.ShapeDtypeStruct(a.shape, a.dtype) for a in arrays],
        20 * grads.size,
        22 * grads.size,
        aliases={3 + len(arrays) + k: k for k in range(had)},
        name="adamw",
    )(grads, grads, grads, *arrays, *so_far)


def solution(mesh):
    group = mesh.shape["dp"]

    def step(x, dy, *arrays):
        weights = arrays[:3]
        layers, rows, width = weights[0].shape
        h0, dy = x[0], dy[0]

        def summed(grads):
            _, n, _, rows, width = grads.shape
            mine = lax.psum_scatter(grads.reshape(group * n * 3 * rows, width), "dp", scatter_dimension=0, tiled=True)
            return mine.reshape(n, 3, rows, width)

        ident = iter(range(100))

        def beside(*pieces, when):
            gather = Gather([(which, layer, chunk, which == 2) for which, layer, chunk in pieces], group)
            return dict(gather=gather, when=when, ident=next(ident), sources=weights)

        wg, wu, wd = ([[None] * CHUNKS for _ in range(layers)] for _ in range(3))

        def keep(got, *pieces):
            for array, (which, layer, chunk) in zip(got, pieces, strict=True):
                (wg, wu, wd)[which][layer][chunk] = array

        pieces = (0, 0, 0), (1, 0, 0)
        extra = beside(*pieces, when=(1, 1))
        keep(fetch(extra["gather"], extra["ident"], weights), *pieces)
        plan = [
            [(0, 0, 1), (1, 0, 1)],
            [(0, 0, 2), (1, 0, 2), (2, 0, 0)],
            [(0, 0, 3), (1, 0, 3), (2, 0, 1)],
            [(2, 0, 2), (2, 0, 3)],
        ]
        ps, gates, ups, a0 = [], [], [], None
        for c in range(CHUNKS):
            got = gate_up(c == 0, h0 if c == 0 else a0, wg[0][c], wu[0][c], **beside(*plan[c], when=(5, 8)))
            if c == 0:
                a0, *got = got
            p, gate, up, *got = got
            keep(got, *plan[c])
            ps.append(p)
            gates.append(gate)
            ups.append(up)
        pieces = [(which, 1, 0) for which in range(3)]
        h1, a1, *got = down(ps, wd[0], h0, **beside(*pieces, when=(4, 6)))
        keep(got, *pieces)
        sums, qs, dgs, dus = [], [], [], []
        for c in range(CHUNKS):
            pieces = [(which, 1, c + 1) for which in range(3)] if c + 1 < CHUNKS else []
            q, dg, du, *got = hidden(a1, dy, wg[1][c], wu[1][c], wd[1][c], **(beside(*pieces, when=(5, 8)) if pieces else {}))
            keep(got, *pieces)
            qs.append(q)
            dgs.append(dg)
            dus.append(du)
        for c in range(CHUNKS):
            sums.append((1, c, summed(by_weights([qs[c]], [dgs[c]], [dus[c]], dy, a1, group, qs[CHUNKS - 2]))))
        dh = by_input(h1, dy, dgs, dus, wg[1], wu[1])
        for c in range(CHUNKS):
            sums.append((0, c, summed(first_back(dh, a0, wd[0][c], gates[c], ups[c], ps[c], group))))
        new = ()
        for layer, start, grads in sums:
            new = adamw(grads, arrays, new, layer, start, group)
        return tuple(new)

    states, cut = P(("rep", "dp"), None, None), P(None, "dp", None)
    return jax.shard_map(
        step,
        mesh=mesh,
        in_specs=(states, states) + (cut,) * 9,
        out_specs=(P("rep", "dp", None),) * 9,
        check_vma=False,
    )
```
